8 devices in a mesh: terms: 8 (over z, y, x, core).
Axes of the slice: x: 2, y: 2, z: 1, core: 2. Of those that a mesh axis runs over, the one named last changes fastest.
Arguments:
- wavefunction: float32 [768, 16, 768], replicated
- left_env: bfloat16 [32, 768, 768], P('terms')
- pair_ops: bfloat16 [32, 16, 16], P('terms')
- right_env: bfloat16 [32, 768, 768], P('terms')
- full_term: int32 [32], P('terms')
Outputs:
- output 1: float32 [7, 768, 16, 768], P(None, 'terms')
- output 2: float32 [6], replicated
- output 3: float32 [6], replicated
All inputs are finite; a program needn't handle non-finite values.
Results may differ from the reference program's by a relative error of at most 0.0114484.
Values are sent between devices in bfloat16 or wider.
A program may use at most 1 GiB of HBM per device.

```python
import jax
import jax.numpy as jnp
from jax import lax

BOND_DIM = 768
PHYS_DIM = 4
TERMS_DEV = 4
NUM_DEV = 8
NUM_TERMS = 32
LANCZOS_STEPS = 6

PAIR_DIM = PHYS_DIM * PHYS_DIM
VEC_SIZE = BOND_DIM * PAIR_DIM * BOND_DIM


def normal_sym(rng_key, num_mats, mat_size):
    raw_draw = jax.random.normal(rng_key, (num_mats, mat_size, mat_size), jnp.float32)
    return (raw_draw + jnp.swapaxes(raw_draw, 1, 2)) * (2.0 * mat_size) ** -0.5


def draw_flags(rng_key):
    count_key, pick_key, order_key = jax.random.split(rng_key, 3)
    block_counts = jax.random.randint(count_key, (NUM_DEV,), 0, TERMS_DEV + 1)
    picked = jax.random.permutation(pick_key, NUM_DEV)
    block_counts = block_counts.at[picked[0]].set(TERMS_DEV).at[picked[1]].set(0)
    rank_table = jax.vmap(lambda sub_key: jax.random.permutation(sub_key, TERMS_DEV))(jax.random.split(order_key, NUM_DEV))
    return (rank_table < block_counts[:, None]).astype(jnp.int32).reshape(NUM_TERMS)


def setup_inputs(seed: int = 0) -> dict:
    wave_key, left_key, pair_key, right_key, flag_key = jax.random.split(jax.random.key(seed), 5)
    diag_shift = (2.0 / NUM_TERMS ** 0.5) ** 0.5
    wavefunction = jax.random.normal(wave_key, (BOND_DIM, PAIR_DIM, BOND_DIM), jnp.float32)
    left_env = (normal_sym(left_key, NUM_TERMS, BOND_DIM) + diag_shift * jnp.eye(BOND_DIM, dtype=jnp.float32)).astype(jnp.bfloat16)
    pair_ops = ((normal_sym(pair_key, NUM_TERMS, PAIR_DIM) + diag_shift * jnp.eye(PAIR_DIM, dtype=jnp.float32)) * NUM_TERMS ** -0.5).astype(jnp.bfloat16)
    right_env = normal_sym(right_key, NUM_TERMS, BOND_DIM).astype(jnp.bfloat16)
    full_term = draw_flags(flag_key)
    return {'wavefunction': wavefunction, 'left_env': left_env, 'pair_ops': pair_ops, 'right_env': right_env, 'full_term': full_term}


def apply_term(vec_bf, term_data):
    left_env, pair_op, right_env, flag_val = term_data
    flat_vec = vec_bf.reshape(BOND_DIM * PAIR_DIM, BOND_DIM)
    right_done = jnp.dot(flat_vec, right_env.T, preferred_element_type=jnp.float32).astype(jnp.bfloat16)
    right_done = jnp.where(flag_val == 1, right_done.reshape(BOND_DIM, PAIR_DIM, BOND_DIM), vec_bf)
    pair_in = right_done.transpose(1, 0, 2).reshape(PAIR_DIM, BOND_DIM * BOND_DIM)
    pair_done = jnp.dot(pair_op, pair_in, preferred_element_type=jnp.float32).astype(jnp.bfloat16)
    left_in = pair_done.reshape(PAIR_DIM, BOND_DIM, BOND_DIM).transpose(1, 0, 2).reshape(BOND_DIM, PAIR_DIM * BOND_DIM)
    return jnp.dot(left_env, left_in, preferred_element_type=jnp.float32).reshape(BOND_DIM, PAIR_DIM, BOND_DIM)


def apply_hamiltonian(vector, left_env, pair_ops, right_env, full_term):
    vec_bf = vector.astype(jnp.bfloat16)

    def add_term(running_sum, term_data):
        return running_sum + apply_term(vec_bf, term_data), None

    start_sum = jnp.zeros((BOND_DIM, PAIR_DIM, BOND_DIM), jnp.float32)
    total_sum, unused = lax.scan(add_term, start_sum, (left_env, pair_ops, right_env, full_term))
    return total_sum


def reference(wavefunction, left_env, pair_ops, right_env, full_term):
    first_vec = wavefunction / jnp.sqrt(jnp.sum(wavefunction * wavefunction) / VEC_SIZE)

    def lanczos_step(state_in, unused):
        current, previous, beta_prev = state_in
        sigma_vec = apply_hamiltonian(current, left_env, pair_ops, right_env, full_term)
        alpha_now = jnp.sum(sigma_vec * current) / VEC_SIZE
        residual = sigma_vec - alpha_now * current - beta_prev * previous
        beta_now = jnp.sqrt(jnp.sum(residual * residual) / VEC_SIZE)
        following = residual / beta_now
        return (following, current, beta_now), (following, alpha_now, beta_now)

    start_state = (first_vec, jnp.zeros_like(first_vec), jnp.zeros((), jnp.float32))
    final_state, outputs = lax.scan(lanczos_step, start_state, None, length=LANCZOS_STEPS)
    vectors, alpha_diag, beta_offdiag = outputs
    krylov = jnp.concatenate([first_vec[None], vectors], axis=0)
    return krylov, alpha_diag, beta_offdiag
```

```python
import functools

import jax
import jax.numpy as jnp
from jax import lax
from jax.experimental import pallas as pl
from jax.experimental.pallas import tpu as pltpu
from jax.sharding import PartitionSpec as P


LANCZOS_STEPS = 6
AXIS_NAME = 'terms'
GROUP = 4
CHUNK = 256
ROW_TILE = 16
BF16 = jnp.bfloat16
F32 = jnp.float32
FIN_BLOCKS = 4


def one_sided_body(order_ref, split_ref, *rest, parts, resume):
    u_refs = rest[:parts]
    pair_ref = rest[parts]
    left_refs = rest[parts + 1:parts + 1 + GROUP * parts]
    rest = rest[parts + 1 + GROUP * parts:]
    if resume:
        sigma_in, rest = rest[0], rest[1:]
    rest = rest[1:]
    sigma_out, _, sigma_ref, z_ref, in_sem, out_sem = rest
    grp = pl.program_id(0)
    nq, nb, nc = u_refs[0].shape
    na = sigma_ref.shape[2]
    half = nq // 2
    last = jnp.maximum(split_ref[0] - 1, 0)

    @pl.when(grp == 0)
    def _():
        if resume:
            copy = pltpu.make_async_copy(sigma_in, sigma_ref, in_sem)
            copy.start()
            copy.wait()
        else:
            sigma_ref[...] = jnp.zeros_like(sigma_ref)

    @pl.when(grp < split_ref[0])
    def _():
        pair = pair_ref[...].reshape(GROUP * nq * ROW_TILE, nq * ROW_TILE)
        for ci in range(parts):
            for bt in range(nb // ROW_TILE):
                rows = pl.ds(bt * ROW_TILE, ROW_TILE)
                y = u_refs[ci][:, rows, :].reshape(nq * ROW_TILE, nc)
                z = jnp.dot(pair, y, preferred_element_type=F32).astype(BF16)
                z = z.reshape(GROUP, nq, ROW_TILE, nc)
                for t in range(GROUP):
                    z_ref[:, rows, (ci * GROUP + t) * nc:(ci * GROUP + t + 1) * nc] = z[t]

    for h in range(2):
        @pl.when(grp < split_ref[0])
        def _():
            left = jnp.concatenate([left_refs[ci * GROUP + t][0] for ci in range(parts) for t in range(GROUP)], axis=0)
            zs = z_ref[h * half:(h + 1) * half].reshape(half * nb, parts * GROUP * nc)
            prod = jnp.dot(zs, left, preferred_element_type=F32).reshape(half, nb, na)
            sigma_ref[h * half:(h + 1) * half] += prod

        @pl.when(grp == last)
        def _():
            pltpu.make_async_copy(sigma_ref.at[pl.ds(h * half, half)], sigma_out.at[pl.ds(h * half, half)], out_sem.at[h]).start()

    @pl.when(grp == last)
    def _():
        for h in range(2):
            pltpu.make_async_copy(sigma_ref.at[pl.ds(h * half, half)], sigma_out.at[pl.ds(h * half, half)], out_sem.at[h]).wait()


def full_body(order_ref, split_ref, u_hbm, right_ref, pair_ref, *rest, gathered):
    left_refs = rest[:GROUP]
    sigma_in, _, sigma_out, _, sigma_ref, u_ref, y_ref, z_ref, u_sem, in_sem, out_sem = rest[GROUP:]
    grp = pl.program_id(0)
    num_grp = pl.num_programs(0)
    nq, nb, na = sigma_ref.shape
    nd = right_ref.shape[2]
    nc = u_ref.shape[-1]
    half = nq // 2

    def u_copy(r):
        if gathered:
            return pltpu.make_async_copy(u_hbm.at[:, r], u_ref.at[:, r], u_sem.at[r])
        return pltpu.make_async_copy(u_hbm.at[r], u_ref.at[r], u_sem.at[r])

    @pl.when((grp == 0) & (split_ref[0] < num_grp))
    def _():
        for r in range(nq):
            u_copy(r).start()
        pltpu.make_async_copy(sigma_in, sigma_ref, in_sem).start()

    @pl.when(grp == split_ref[0])
    def _():
        for r in range(nq):
            u_copy(r).wait()

    @pl.when(grp >= split_ref[0])
    def _():
        right = right_ref[...].reshape(GROUP * nb, nd)
        for r in range(nq):
            u = (u_ref[:, r] if gathered else u_ref[r]).reshape(nd, nc)
            y_ref[r] = jnp.dot(right, u, preferred_element_type=F32).astype(BF16)
        for t in range(GROUP):
            for bt in range(nb // ROW_TILE):
                y = y_ref[:, pl.ds(t * nb + bt * ROW_TILE, ROW_TILE), :].reshape(nq * ROW_TILE, nc)
                z = jnp.dot(pair_ref[t], y, preferred_element_type=F32).astype(BF16)
                z_ref[:, pl.ds(bt * ROW_TILE, ROW_TILE), t * nc:(t + 1) * nc] = z.reshape(nq, ROW_TILE, nc)

    @pl.when(grp == split_ref[0])
    def _():
        pltpu.make_async_copy(sigma_in, sigma_ref, in_sem).wait()

    for h in range(2):
        @pl.when(grp >= split_ref[0])
        def _():
            left = jnp.concatenate([left_refs[t][0] for t in range(GROUP)], axis=0)
            zs = z_ref[h * half:(h + 1) * half].reshape(half * nb, GROUP * nc)
            prod = jnp.dot(zs, left, preferred_element_type=F32).reshape(half, nb, na)
            sigma_ref[h * half:(h + 1) * half] += prod

        @pl.when((grp == num_grp - 1) & (split_ref[0] < num_grp))
        def _():
            pltpu.make_async_copy(sigma_ref.at[pl.ds(h * half, half)], sigma_out.at[pl.ds(h * half, half)], out_sem.at[h]).start()

    @pl.when((grp == num_grp - 1) & (split_ref[0] < num_grp))
    def _():
        for h in range(2):
            pltpu.make_async_copy(sigma_ref.at[pl.ds(h * half, half)], sigma_out.at[pl.ds(h * half, half)], out_sem.at[h]).wait()


ANY = pl.BlockSpec(memory_space=pl.ANY)
VMEM_LIMIT = 63 << 20


def whole(shape):
    return pl.BlockSpec(shape, lambda g, o, s: (0,) * len(shape), pipeline_mode=pl.Buffered(1))


def one_sided_call(order, split, u_parts, pair_blk, left_parts, carried, sigma=None):
    parts = len(u_parts)
    nq, nb, nc = u_parts[0].shape
    na = left_parts[0].shape[2]
    terms = pair_blk.shape[0]
    nk = nq * ROW_TILE

    def clamp(g, s):
        return jnp.minimum(g, jnp.maximum(s[0] - 1, 0))

    left_specs = [pl.BlockSpec((1, nc, na), functools.partial(lambda g, o, s, t: (o[clamp(g, s) * GROUP + t], 0, 0), t=t))
                  for _ in range(parts) for t in range(GROUP)]
    resume = sigma is not None
    n = terms // 2
    first = 2 + parts + 1 + GROUP * parts
    aliases = {first: 0, first + 1: 1} if resume else {first: 1}
    return pl.pallas_call(
        functools.partial(one_sided_body, parts=parts, resume=resume),
        grid_spec=pltpu.PrefetchScalarGridSpec(
            num_scalar_prefetch=2, grid=(terms // GROUP,),
            in_specs=[whole((nq, nb, nc))] * parts + [pl.BlockSpec((GROUP, nk, nk), lambda g, o, s: (clamp(g, s), 0, 0))] + left_specs
            + [ANY] * (2 if resume else 1),
            out_specs=[ANY, ANY],
            scratch_shapes=[pltpu.VMEM((nq, nb, na), F32), pltpu.VMEM((nq, nb, parts * GROUP * nc), BF16),
                            pltpu.SemaphoreType.DMA, pltpu.SemaphoreType.DMA((2,))]),
        out_shape=[jax.ShapeDtypeStruct((nq, nb, na), F32), jax.ShapeDtypeStruct(carried.shape, carried.dtype)],
        input_output_aliases=aliases,
        compiler_params=pltpu.CompilerParams(dimension_semantics=('arbitrary',), vmem_limit_bytes=VMEM_LIMIT),
        cost_estimate=pl.CostEstimate(flops=n * 2 * nq * nb * parts * nc * (na + nk), bytes_accessed=n * na * nc * parts * 2, transcendentals=0),
        name='one_sided',
    )(order, split, *u_parts, pair_blk, *[left_parts[c] for c in range(parts) for _ in range(GROUP)], *([sigma] if resume else []), carried)


def full_call(order, split, u_part, right_slab, pair_blk, left_part, sigma, carried):
    nq, nb, na = sigma.shape
    nc = u_part.shape[-1]
    terms, _, nd = right_slab.shape
    nk = nq * ROW_TILE

    def at_least(g, s):
        return jnp.minimum(jnp.maximum(g, s[0]), terms // GROUP - 1)

    left_specs = [pl.BlockSpec((1, nc, na), functools.partial(lambda g, o, s, t: (o[at_least(g, s) * GROUP + t], 0, 0), t=t))
                  for t in range(GROUP)]
    n = terms // 2
    return pl.pallas_call(
        functools.partial(full_body, gathered=u_part.ndim == 4),
        grid_spec=pltpu.PrefetchScalarGridSpec(
            num_scalar_prefetch=2, grid=(terms // GROUP,),
            in_specs=[ANY,
                      pl.BlockSpec((GROUP, nb, nd), lambda g, o, s: (at_least(g, s), 0, 0)),
                      pl.BlockSpec((GROUP, nk, nk), lambda g, o, s: (at_least(g, s), 0, 0))] + left_specs + [ANY, ANY],
            out_specs=[ANY, ANY],
            scratch_shapes=[pltpu.VMEM((nq, nb, na), F32), pltpu.VMEM(u_part.shape, BF16),
                            pltpu.VMEM((nq, GROUP * nb, nc), BF16), pltpu.VMEM((nq, nb, GROUP * nc), BF16),
                            pltpu.SemaphoreType.DMA((nq,)), pltpu.SemaphoreType.DMA, pltpu.SemaphoreType.DMA((2,))]),
        out_shape=[jax.ShapeDtypeStruct((nq, nb, na), F32), jax.ShapeDtypeStruct(carried.shape, carried.dtype)],
        input_output_aliases={2 + 3 + GROUP: 0, 2 + 4 + GROUP: 1},
        compiler_params=pltpu.CompilerParams(dimension_semantics=('arbitrary',), vmem_limit_bytes=VMEM_LIMIT),
        cost_estimate=pl.CostEstimate(flops=n * 2 * nq * nb * nc * (nd + na + nk), bytes_accessed=n * na * nc * 2 + u_part.size * 2, transcendentals=0),
        name='full_terms',
    )(order, split, u_part, right_slab, pair_blk, *[left_part] * GROUP, sigma, carried)


def place_body(*refs, num, width):
    x_ref, out_ref = refs[0], refs[-1]
    for src in range(num):
        out_ref[0, :, :, src * width:(src + 1) * width] = x_ref[src]


def place_call(arrived, krylov, index):
    num, rows, nq, width = arrived.shape
    blk = rows // 4
    return pl.pallas_call(
        functools.partial(place_body, num=num, width=width),
        grid=(4,),
        in_specs=[pl.BlockSpec((num, blk, nq, width), lambda i: (0, i, 0, 0)), ANY],
        out_specs=pl.BlockSpec((1, blk, nq, num * width), lambda i: (index, i, 0, 0)),
        out_shape=jax.ShapeDtypeStruct(krylov.shape, krylov.dtype),
        input_output_aliases={1: 0},
        compiler_params=pltpu.CompilerParams(dimension_semantics=('arbitrary',), vmem_limit_bytes=VMEM_LIMIT),
        cost_estimate=pl.CostEstimate(flops=0, bytes_accessed=8 * arrived.size, transcendentals=0),
        name='place',
    )(arrived, krylov)


def first_body(me_ref, norm_ref, psi_ref, out_ref):
    out_ref[0] = psi_ref[...] / norm_ref[:1, :1]


def first_call(wavefunction, norm_tile, me, rows, count):
    _, nq, width = wavefunction.shape
    blk = rows // 4
    return pl.pallas_call(
        first_body,
        grid_spec=pltpu.PrefetchScalarGridSpec(
            num_scalar_prefetch=1, grid=(4,),
            in_specs=[pl.BlockSpec((8, 128), lambda i, m: (0, 0)), pl.BlockSpec((blk, nq, width), lambda i, m: (m[0] * 4 + i, 0, 0))],
            out_specs=pl.BlockSpec((1, blk, nq, width), lambda i, m: (0, i, 0, 0))),
        out_shape=jax.ShapeDtypeStruct((count, rows, nq, width), F32),
        compiler_params=pltpu.CompilerParams(dimension_semantics=('arbitrary',), vmem_limit_bytes=VMEM_LIMIT),
        cost_estimate=pl.CostEstimate(flops=rows * nq * width, bytes_accessed=8 * rows * nq * width, transcendentals=0),
        name='first',
    )(me, norm_tile, wavefunction)


def exchange_body(x_ref, out_ref, send_sem, recv_sem, *, num):
    me = lax.axis_index(AXIS_NAME)
    barrier = pltpu.get_barrier_semaphore()
    for off in range(1, num):
        pl.semaphore_signal(barrier, inc=1, device_id=(lax.rem(me + off, num),), device_id_type=pl.DeviceIdType.MESH)
    pl.semaphore_wait(barrier, num - 1)
    copies = []
    for off in range(1, num):
        copies.append(pltpu.make_async_remote_copy(
            src_ref=x_ref, dst_ref=out_ref.at[me], send_sem=send_sem.at[off - 1], recv_sem=recv_sem.at[off - 1],
            device_id=(lax.rem(me + off, num),), device_id_type=pl.DeviceIdType.MESH))
    for copy in copies:
        copy.start()
    out_ref[me] = x_ref[...]
    for copy in copies:
        copy.wait()


def exchange_call(x, num):
    vmem = pl.BlockSpec(memory_space=pltpu.VMEM)
    return pl.pallas_call(
        functools.partial(exchange_body, num=num), in_specs=[vmem], out_specs=vmem,
        out_shape=jax.ShapeDtypeStruct((num,) + x.shape, x.dtype),
        scratch_shapes=[pltpu.SemaphoreType.DMA((num - 1,))] * 2,
        compiler_params=pltpu.CompilerParams(collective_id=20, has_side_effects=True, vmem_limit_bytes=VMEM_LIMIT),
        name='exchange')(x)


def sum_over_devices(slot_ref, value, send_sem, recv_sem, me, num):
    slot_ref[me] = value
    copies = []
    for off in range(1, num):
        peer = lax.rem(me + off, num)
        copies.append(pltpu.make_async_remote_copy(
            src_ref=slot_ref.at[me], dst_ref=slot_ref.at[me], send_sem=send_sem.at[off - 1], recv_sem=recv_sem.at[off - 1],
            device_id=(peer,), device_id_type=pl.DeviceIdType.MESH))
    for copy in copies:
        copy.start()
    for copy in copies:
        copy.wait()
    total = slot_ref[0]
    for src in range(1, num):
        total = total + slot_ref[src]
    return jnp.sum(total)


def fold(prod):
    rows, cols = prod.shape
    part = jnp.sum(prod.reshape(rows // 8, 8, cols), axis=0)
    out = part[:, :128]
    for i in range(1, cols // 128):
        out = out + part[:, i * 128:(i + 1) * 128]
    return out


def finish_body(beta_prev_ref, sigma_hbm, cur_hbm, prev_hbm, next_hbm, u0, u1, u2, alpha_ref, beta_ref,
                sigma_ref, cur_ref, prev_ref, low_ref, slot_a, slot_b, in_sem, out_sem, send_a, recv_a, send_b, recv_b, *, num, vec_size):
    me = lax.axis_index(AXIS_NAME)
    nq, _, _ = sigma_ref.shape
    blk = nq // FIN_BLOCKS

    def load(n, i):
        src, dst = ((sigma_hbm, sigma_ref), (cur_hbm, cur_ref), (prev_hbm, prev_ref))[n]
        rows = pl.ds(i * blk, blk)
        return pltpu.make_async_copy(src.at[rows], dst.at[rows], in_sem.at[n, i])

    for i in range(FIN_BLOCKS):
        load(0, i).start()
        load(1, i).start()
    for i in range(FIN_BLOCKS):
        load(2, i).start()
    barrier = pltpu.get_barrier_semaphore()
    for off in range(1, num):
        pl.semaphore_signal(barrier, inc=1, device_id=(lax.rem(me + off, num),), device_id_type=pl.DeviceIdType.MESH)

    part = jnp.zeros((8, 128), F32)
    for i in range(FIN_BLOCKS):
        load(0, i).wait()
        load(1, i).wait()
        part = lax.fori_loop(i * blk, (i + 1) * blk, lambda q, acc: acc + fold(sigma_ref[q] * cur_ref[q]), part)
    pl.semaphore_wait(barrier, num - 1)
    alpha = sum_over_devices(slot_a, part, send_a, recv_a, me, num) / vec_size
    beta_prev = beta_prev_ref[0]
    for i in range(FIN_BLOCKS):
        load(2, i).wait()

    def residual_part(q, acc):
        res = sigma_ref[q] - alpha * cur_ref[q] - beta_prev * prev_ref[q]
        sigma_ref[q] = res
        return acc + fold(res * res)

    part = lax.fori_loop(0, nq, residual_part, jnp.zeros((8, 128), F32))
    norm = sum_over_devices(slot_b, part, send_b, recv_b, me, num) / vec_size
    beta_vec = jnp.sqrt(jnp.full((8, 128), norm, F32))
    alpha_ref[...] = jnp.full((8, 128), alpha, F32)
    beta_ref[...] = beta_vec
    beta_row = beta_vec[:1, :1]

    def scale_part(q, carry):
        nxt = sigma_ref[q] / beta_row
        cur_ref[q] = nxt
        low_ref[q] = nxt.astype(BF16)
        return carry

    def stores(i):
        rows = pl.ds(i * blk, blk)
        return [pltpu.make_async_copy(cur_ref.at[rows], next_hbm.at[rows], out_sem.at[0, i])] + [
            pltpu.make_async_copy(low_ref.at[rows, :, pl.ds(n * CHUNK, CHUNK)], ref.at[rows], out_sem.at[1 + n, i])
            for n, ref in enumerate((u0, u1, u2))]

    for i in range(FIN_BLOCKS):
        lax.fori_loop(i * blk, (i + 1) * blk, scale_part, 0)
        for copy in stores(i):
            copy.start()
    for i in range(FIN_BLOCKS):
        for copy in stores(i):
            copy.wait()


def finish_call(beta_prev, sigma, cur, prev, num, vec_size, call_id):
    nq, nb, na = sigma.shape
    vmem = pl.BlockSpec(memory_space=pltpu.VMEM)
    return pl.pallas_call(
        functools.partial(finish_body, num=num, vec_size=vec_size),
        in_specs=[pl.BlockSpec(memory_space=pltpu.SMEM)] + [ANY] * 3,
        out_specs=[ANY] * 4 + [vmem] * 2,
        out_shape=[jax.ShapeDtypeStruct((nq, nb, na), F32)] + [jax.ShapeDtypeStruct((nq, nb, CHUNK), BF16)] * 3
        + [jax.ShapeDtypeStruct((8, 128), F32)] * 2,
        scratch_shapes=[pltpu.VMEM((nq, nb, na), F32)] * 3 + [pltpu.VMEM((nq, nb, na), BF16)] + [pltpu.VMEM((num, 8, 128), F32)] * 2
        + [pltpu.SemaphoreType.DMA((3, FIN_BLOCKS)), pltpu.SemaphoreType.DMA((4, FIN_BLOCKS))] + [pltpu.SemaphoreType.DMA((num - 1,))] * 4,
        compiler_params=pltpu.CompilerParams(collective_id=call_id, has_side_effects=True, vmem_limit_bytes=VMEM_LIMIT),
        cost_estimate=pl.CostEstimate(flops=10 * sigma.size, bytes_accessed=22 * sigma.size, transcendentals=0),
        name='finish',
    )(beta_prev, sigma, cur, prev)


def solution(mesh):
    num = mesh.shape[AXIS_NAME]

    def device_body(wavefunction, left_loc, pair_loc, right_loc, flag_loc):
        bond, nq, _ = wavefunction.shape
        vec_size = wavefunction.size
        slab = bond // num
        me = lax.axis_index(AXIS_NAME)
        nchunk = bond // CHUNK

        terms_loc = pair_loc.shape[0]
        small = jnp.concatenate([pair_loc.astype(F32).reshape(8, 128), jnp.pad(flag_loc.astype(F32), (0, 1024 - terms_loc)).reshape(8, 128)])
        small_all = exchange_call(small, num)
        right_slab = lax.all_to_all(right_loc, AXIS_NAME, split_axis=1, concat_axis=0, tiled=True)
        left_parts = []
        for i in range(nchunk):
            left_parts.append(lax.all_gather(left_loc[:, i * CHUNK:(i + 1) * CHUNK], AXIS_NAME, axis=0, tiled=True))
        pair_all = small_all[:, :8].reshape(num * terms_loc, nq, nq).astype(BF16)
        flags = small_all[:, 8, :terms_loc].reshape(-1).astype(jnp.int32)
        order = jnp.argsort(flags, stable=True).astype(jnp.int32)
        split = ((flags.shape[0] - jnp.sum(flags)) // GROUP).astype(jnp.int32).reshape(1)
        unit = (jnp.arange(slab)[:, None] + me * slab == jnp.arange(bond)[None, :]).astype(BF16)
        right_slab = jnp.where(flags[:, None, None] == 1, right_slab, unit[None])[order]
        eye = jnp.eye(ROW_TILE, dtype=BF16)
        pair_sorted = pair_all[order]
        pair_blk = (pair_sorted[:, :, None, :, None] * eye[None, None, :, None, :]).reshape(-1, nq * ROW_TILE, nq * ROW_TILE)

        norm0 = jnp.sqrt(jnp.sum(wavefunction * wavefunction) / vec_size)
        krylov = first_call(wavefunction, jnp.full((8, 128), norm0, F32), me.reshape(1).astype(jnp.int32), slab, LANCZOS_STEPS + 1)
        cur = (lax.dynamic_slice_in_dim(wavefunction, me * slab, slab, axis=2) / norm0).transpose(1, 2, 0)
        cur_low = cur.astype(BF16)
        u_parts = [cur_low[:, :, i * CHUNK:(i + 1) * CHUNK] for i in range(nchunk)]
        whole_low = (wavefunction / norm0).astype(BF16).transpose(1, 2, 0)
        u_wide = [whole_low[:, :, i * CHUNK:(i + 1) * CHUNK] for i in range(nchunk)]
        prev = jnp.zeros_like(cur)
        beta_prev = jnp.zeros((1,), F32)
        tiles = []
        leaving = arriving = None
        for step in range(LANCZOS_STEPS):
            if step == 0:
                sigma = None
                for i in range(nchunk):
                    sigma, krylov = one_sided_call(order, split, u_parts[i:i + 1], pair_blk, left_parts[i:i + 1], krylov, sigma)
                    sigma, krylov = full_call(order, split, u_wide[i], right_slab, pair_blk, left_parts[i], sigma, krylov)
            else:
                if arriving is None:
                    sigma, krylov = one_sided_call(order, split, u_parts, pair_blk, left_parts, krylov)
                else:
                    sigma, arriving = one_sided_call(order, split, u_parts, pair_blk, left_parts, arriving)
                    krylov = place_call(arriving, krylov, step - 1)
                sigma, krylov = full_call(order, split, u_wide[0], right_slab, pair_blk, left_parts[0], sigma, krylov)
                sigma, leaving = full_call(order, split, u_wide[1], right_slab, pair_blk, left_parts[1], sigma, leaving)
                arriving = lax.all_to_all(leaving, AXIS_NAME, split_axis=0, concat_axis=0, tiled=False)
                sigma, krylov = full_call(order, split, u_wide[2], right_slab, pair_blk, left_parts[2], sigma, krylov)
            nxt, *u_parts, alpha_t, beta_t = finish_call(beta_prev, sigma, cur, prev, num, vec_size, step)
            beta_prev = beta_t[0, :1]
            tiles += [alpha_t[0, :1], beta_prev]
            if step + 1 < LANCZOS_STEPS:
                u_wide = [lax.all_gather(part, AXIS_NAME, axis=0, tiled=False) for part in u_parts]
            prev, cur = cur, nxt
            leaving = nxt.transpose(2, 0, 1).reshape(num, slab, nq, slab)
        krylov = place_call(arriving, krylov, LANCZOS_STEPS - 1)
        arriving = lax.all_to_all(leaving, AXIS_NAME, split_axis=0, concat_axis=0, tiled=False)
        krylov = place_call(arriving, krylov, LANCZOS_STEPS)
        scalars = jnp.concatenate(tiles)
        return krylov, scalars[0::2], scalars[1::2]

    return jax.shard_map(device_body, mesh=mesh, in_specs=(P(), P(AXIS_NAME), P(AXIS_NAME), P(AXIS_NAME), P(AXIS_NAME)), out_specs=(P(None, AXIS_NAME), P(), P()), check_vma=False)
```

```python
import functools

import jax
import jax.numpy as jnp
from jax import lax
from jax.experimental import pallas as pl
from jax.experimental.pallas import tpu as pltpu
from jax.sharding import PartitionSpec as P


LANCZOS_STEPS = 6
AXIS_NAME = 'terms'
GROUP = 4
CHUNK = 384
ROW_TILE = 16
BF16 = jnp.bfloat16
F32 = jnp.float32
FIN_BLOCKS = 4


def one_sided_body(order_ref, split_ref, *rest, parts, resume):
    u_refs = rest[:parts]
    pair_ref = rest[parts]
    left_refs = rest[parts + 1:parts + 1 + GROUP * parts]
    rest = rest[parts + 1 + GROUP * parts:]
    if resume:
        sigma_in, rest = rest[0], rest[1:]
    rest = rest[1:]
    sigma_out, _, sigma_ref, z_ref, in_sem, out_sem = rest
    grp = pl.program_id(0)
    nq, nb, nc = u_refs[0].shape
    na = sigma_ref.shape[2]
    half = nq // 2
    last = jnp.maximum(split_ref[0] - 1, 0)

    @pl.when(grp == 0)
    def _():
        if resume:
            copy = pltpu.make_async_copy(sigma_in, sigma_ref, in_sem)
            copy.start()
            copy.wait()
        else:
            sigma_ref[...] = jnp.zeros_like(sigma_ref)

    @pl.when(grp < split_ref[0])
    def _():
        pair = pair_ref[...].reshape(GROUP * nq * ROW_TILE, nq * ROW_TILE)
        for ci in range(parts):
            for bt in range(0, nb // ROW_TILE, 2):
                rows = [pl.ds((bt + k) * ROW_TILE, ROW_TILE) for k in range(2)]
                y = jnp.concatenate([u_refs[ci][:, rows[k], :].reshape(nq * ROW_TILE, nc) for k in range(2)], axis=1)
                z = jnp.dot(pair, y, preferred_element_type=F32).astype(BF16)
                for k in range(2):
                    part = z[:, k * nc:(k + 1) * nc].reshape(GROUP, nq, ROW_TILE, nc)
                    for t in range(GROUP):
                        z_ref[:, rows[k], (ci * GROUP + t) * nc:(ci * GROUP + t + 1) * nc] = part[t]

    for h in range(2):
        @pl.when(grp < split_ref[0])
        def _():
            left = jnp.concatenate([left_refs[ci * GROUP + t][0] for ci in range(parts) for t in range(GROUP)], axis=0)
            zs = z_ref[h * half:(h + 1) * half].reshape(half * nb, parts * GROUP * nc)
            prod = jnp.dot(zs, left, preferred_element_type=F32).reshape(half, nb, na)
            sigma_ref[h * half:(h + 1) * half] += prod

        @pl.when(grp == last)
        def _():
            pltpu.make_async_copy(sigma_ref.at[pl.ds(h * half, half)], sigma_out.at[pl.ds(h * half, half)], out_sem.at[h]).start()

    @pl.when(grp == last)
    def _():
        for h in range(2):
            pltpu.make_async_copy(sigma_ref.at[pl.ds(h * half, half)], sigma_out.at[pl.ds(h * half, half)], out_sem.at[h]).wait()


def full_body(order_ref, split_ref, u_hbm, right_ref, pair_ref, *rest, gathered, chunk):
    left_refs = rest[:GROUP]
    sigma_in, _, sigma_out, _, sigma_ref, u_ref, y_ref, z_ref, u_sem, in_sem, out_sem = rest[GROUP:]
    grp = pl.program_id(0)
    num_grp = pl.num_programs(0)
    nq, nb, na = sigma_ref.shape
    nd = right_ref.shape[2]
    nc = u_ref.shape[-1]
    half = nq // 2

    def u_copy(r):
        cols = pl.ds(chunk * nc, nc)
        if gathered:
            return pltpu.make_async_copy(u_hbm.at[:, r, :, cols], u_ref.at[:, r], u_sem.at[r])
        return pltpu.make_async_copy(u_hbm.at[r, :, cols], u_ref.at[r], u_sem.at[r])

    @pl.when((grp == 0) & (split_ref[0] < num_grp))
    def _():
        for r in range(nq):
            u_copy(r).start()
        pltpu.make_async_copy(sigma_in, sigma_ref, in_sem).start()

    def stage_right(first, last):
        right = right_ref[...].reshape(GROUP * nb, nd)
        for r in range(first, last, 2):
            u = jnp.concatenate([(u_ref[:, r + k] if gathered else u_ref[r + k]).reshape(nd, nc) for k in range(2)], axis=1)
            y = jnp.dot(right, u, preferred_element_type=F32).astype(BF16)
            for k in range(2):
                y_ref[r + k] = y[:, k * nc:(k + 1) * nc]

    head = nq // 4

    @pl.when(grp == split_ref[0])
    def _():
        for r in range(head):
            u_copy(r).wait()

    @pl.when(grp >= split_ref[0])
    def _():
        stage_right(0, head)

    @pl.when(grp == split_ref[0])
    def _():
        for r in range(head, nq):
            u_copy(r).wait()

    @pl.when(grp >= split_ref[0])
    def _():
        stage_right(head, nq)
        for t in range(GROUP):
            for bt in range(0, nb // ROW_TILE, 2):
                y = jnp.concatenate([y_ref[:, pl.ds(t * nb + (bt + k) * ROW_TILE, ROW_TILE), :].reshape(nq * ROW_TILE, nc) for k in range(2)], axis=1)
                z = jnp.dot(pair_ref[t], y, preferred_element_type=F32).astype(BF16)
                for k in range(2):
                    z_ref[:, pl.ds((bt + k) * ROW_TILE, ROW_TILE), t * nc:(t + 1) * nc] = z[:, k * nc:(k + 1) * nc].reshape(nq, ROW_TILE, nc)

    @pl.when(grp == split_ref[0])
    def _():
        pltpu.make_async_copy(sigma_in, sigma_ref, in_sem).wait()

    for h in range(2):
        @pl.when(grp >= split_ref[0])
        def _():
            left = jnp.concatenate([left_refs[t][0] for t in range(GROUP)], axis=0)
            zs = z_ref[h * half:(h + 1) * half].reshape(half * nb, GROUP * nc)
            prod = jnp.dot(zs, left, preferred_element_type=F32).reshape(half, nb, na)
            sigma_ref[h * half:(h + 1) * half] += prod

        @pl.when((grp == num_grp - 1) & (split_ref[0] < num_grp))
        def _():
            pltpu.make_async_copy(sigma_ref.at[pl.ds(h * half, half)], sigma_out.at[pl.ds(h * half, half)], out_sem.at[h]).start()

    @pl.when((grp == num_grp - 1) & (split_ref[0] < num_grp))
    def _():
        for h in range(2):
            pltpu.make_async_copy(sigma_ref.at[pl.ds(h * half, half)], sigma_out.at[pl.ds(h * half, half)], out_sem.at[h]).wait()


ANY = pl.BlockSpec(memory_space=pl.ANY)
VMEM_LIMIT = 63 << 20


def one_sided_call(order, split, u_parts, pair_blk, left_parts, carried, sigma=None):
    parts = len(u_parts)
    nq, nb, _ = u_parts[0][0].shape
    nc = CHUNK
    na = left_parts[0].shape[2]
    terms = pair_blk.shape[0]
    nk = nq * ROW_TILE

    def clamp(g, s):
        return jnp.minimum(g, jnp.maximum(s[0] - 1, 0))

    left_specs = [pl.BlockSpec((1, nc, na), functools.partial(lambda g, o, s, t: (o[clamp(g, s) * GROUP + t], 0, 0), t=t))
                  for _ in range(parts) for t in range(GROUP)]
    resume = sigma is not None
    n = terms // 2
    first = 2 + parts + 1 + GROUP * parts
    aliases = {first: 0, first + 1: 1} if resume else {first: 1}
    return pl.pallas_call(
        functools.partial(one_sided_body, parts=parts, resume=resume),
        grid_spec=pltpu.PrefetchScalarGridSpec(
            num_scalar_prefetch=2, grid=(terms // GROUP,),
            in_specs=[pl.BlockSpec((nq, nb, nc), functools.partial(lambda g, o, s, c: (0, 0, c), c=c), pipeline_mode=pl.Buffered(1)) for _, c in u_parts]
            + [pl.BlockSpec((GROUP, nk, nk), lambda g, o, s: (clamp(g, s), 0, 0))] + left_specs
            + [ANY] * (2 if resume else 1),
            out_specs=[ANY, ANY],
            scratch_shapes=[pltpu.VMEM((nq, nb, na), F32), pltpu.VMEM((nq, nb, parts * GROUP * nc), BF16),
                            pltpu.SemaphoreType.DMA, pltpu.SemaphoreType.DMA((2,))]),
        out_shape=[jax.ShapeDtypeStruct((nq, nb, na), F32), jax.ShapeDtypeStruct(carried.shape, carried.dtype)],
        input_output_aliases=aliases,
        compiler_params=pltpu.CompilerParams(dimension_semantics=('arbitrary',), vmem_limit_bytes=VMEM_LIMIT),
        cost_estimate=pl.CostEstimate(flops=n * 2 * nq * nb * parts * nc * (na + nk), bytes_accessed=n * na * nc * parts * 2, transcendentals=0),
        name='one_sided',
    )(order, split, *[u for u, _ in u_parts], pair_blk, *[left_parts[c] for c in range(parts) for _ in range(GROUP)], *([sigma] if resume else []), carried)


def full_call(order, split, u_part, chunk, right_slab, pair_blk, left_part, sigma, carried):
    nq, nb, na = sigma.shape
    nc = CHUNK
    terms, _, nd = right_slab.shape
    nk = nq * ROW_TILE

    def at_least(g, s):
        return jnp.minimum(jnp.maximum(g, s[0]), terms // GROUP - 1)

    left_specs = [pl.BlockSpec((1, nc, na), functools.partial(lambda g, o, s, t: (o[at_least(g, s) * GROUP + t], 0, 0), t=t))
                  for t in range(GROUP)]
    n = terms // 2
    return pl.pallas_call(
        functools.partial(full_body, gathered=u_part.ndim == 4, chunk=chunk),
        grid_spec=pltpu.PrefetchScalarGridSpec(
            num_scalar_prefetch=2, grid=(terms // GROUP,),
            in_specs=[ANY,
                      pl.BlockSpec((GROUP, nb, nd), lambda g, o, s: (at_least(g, s), 0, 0)),
                      pl.BlockSpec((GROUP, nk, nk), lambda g, o, s: (at_least(g, s), 0, 0))] + left_specs + [ANY, ANY],
            out_specs=[ANY, ANY],
            scratch_shapes=[pltpu.VMEM((nq, nb, na), F32), pltpu.VMEM(u_part.shape[:-1] + (nc,), BF16),
                            pltpu.VMEM((nq, GROUP * nb, nc), BF16), pltpu.VMEM((nq, nb, GROUP * nc), BF16),
                            pltpu.SemaphoreType.DMA((nq,)), pltpu.SemaphoreType.DMA, pltpu.SemaphoreType.DMA((2,))]),
        out_shape=[jax.ShapeDtypeStruct((nq, nb, na), F32), jax.ShapeDtypeStruct(carried.shape, carried.dtype)],
        input_output_aliases={2 + 3 + GROUP: 0, 2 + 4 + GROUP: 1},
        compiler_params=pltpu.CompilerParams(dimension_semantics=('arbitrary',), vmem_limit_bytes=VMEM_LIMIT),
        cost_estimate=pl.CostEstimate(flops=n * 2 * nq * nb * nc * (nd + na + nk), bytes_accessed=n * na * nc * 2 + nq * nd * nc * 2, transcendentals=0),
        name='full_terms',
    )(order, split, u_part, right_slab, pair_blk, *[left_part] * GROUP, sigma, carried)


def place_body(*refs, num, nq, width):
    x_ref, out_ref = refs[0], refs[-1]
    for q0 in range(0, nq, 8):
        lines = [jnp.concatenate([x_ref[src, :, q * width:(q + 1) * width] for src in range(num)], axis=1) for q in range(q0, q0 + 8)]
        out_ref[0, :, q0:q0 + 8, :] = jnp.swapaxes(jnp.stack(lines, axis=0), 0, 1)


def place_call(arrived, krylov, index):
    num, rows, size = arrived.shape
    nq, wide = krylov.shape[2:]
    blk = rows // 4
    return pl.pallas_call(
        functools.partial(place_body, num=num, nq=nq, width=wide // num),
        grid=(4,),
        in_specs=[pl.BlockSpec((num, blk, size), lambda i: (0, i, 0)), ANY],
        out_specs=pl.BlockSpec((1, blk, nq, wide), lambda i: (index, i, 0, 0)),
        out_shape=jax.ShapeDtypeStruct(krylov.shape, krylov.dtype),
        input_output_aliases={1: 0},
        compiler_params=pltpu.CompilerParams(dimension_semantics=('arbitrary',), vmem_limit_bytes=VMEM_LIMIT),
        cost_estimate=pl.CostEstimate(flops=0, bytes_accessed=8 * arrived.size, transcendentals=0),
        name='place',
    )(arrived, krylov)


def first_body(me_ref, norm_ref, psi_ref, out_ref):
    out_ref[0] = psi_ref[...] / norm_ref[:1, :1]


def first_call(wavefunction, norm_tile, me, rows, count):
    _, nq, width = wavefunction.shape
    blk = rows // 4
    return pl.pallas_call(
        first_body,
        grid_spec=pltpu.PrefetchScalarGridSpec(
            num_scalar_prefetch=1, grid=(4,),
            in_specs=[pl.BlockSpec((8, 128), lambda i, m: (0, 0)), pl.BlockSpec((blk, nq, width), lambda i, m: (m[0] * 4 + i, 0, 0))],
            out_specs=pl.BlockSpec((1, blk, nq, width), lambda i, m: (0, i, 0, 0))),
        out_shape=jax.ShapeDtypeStruct((count, rows, nq, width), F32),
        compiler_params=pltpu.CompilerParams(dimension_semantics=('arbitrary',), vmem_limit_bytes=VMEM_LIMIT),
        cost_estimate=pl.CostEstimate(flops=rows * nq * width, bytes_accessed=8 * rows * nq * width, transcendentals=0),
        name='first',
    )(me, norm_tile, wavefunction)


def exchange_body(x_ref, psi_hbm, out_ref, norm_ref, stage_ref, psi_ref, psi_sem, send_sem, recv_sem, *, num, vec_size):
    me = lax.axis_index(AXIS_NAME)
    rows = psi_ref.shape[0]
    blk = rows // FIN_BLOCKS
    small = x_ref.shape[0]

    def load(i):
        return pltpu.make_async_copy(psi_hbm.at[pl.ds(me * rows + i * blk, blk)], psi_ref.at[pl.ds(i * blk, blk)], psi_sem.at[i])

    for i in range(FIN_BLOCKS):
        load(i).start()
    barrier = pltpu.get_barrier_semaphore()
    for off in range(1, num):
        pl.semaphore_signal(barrier, inc=1, device_id=(lax.rem(me + off, num),), device_id_type=pl.DeviceIdType.MESH)
    stage_ref[:small] = x_ref[...]
    part = jnp.zeros((8, 128), F32)
    for i in range(FIN_BLOCKS):
        load(i).wait()
        part = lax.fori_loop(i * blk, (i + 1) * blk, lambda a, acc: acc + fold(psi_ref[a] * psi_ref[a]), part)
    stage_ref[small:] = part
    pl.semaphore_wait(barrier, num - 1)
    copies = []
    for off in range(1, num):
        copies.append(pltpu.make_async_remote_copy(
            src_ref=stage_ref, dst_ref=out_ref.at[me], send_sem=send_sem.at[off - 1], recv_sem=recv_sem.at[off - 1],
            device_id=(lax.rem(me + off, num),), device_id_type=pl.DeviceIdType.MESH))
    for copy in copies:
        copy.start()
    out_ref[me] = stage_ref[...]
    for copy in copies:
        copy.wait()
    total = out_ref[0, small:]
    for src in range(1, num):
        total = total + out_ref[src, small:]
    norm_ref[...] = jnp.sqrt(jnp.full((8, 128), jnp.sum(total) / vec_size, F32))


def exchange_call(x, wavefunction, num):
    vmem = pl.BlockSpec(memory_space=pltpu.VMEM)
    bond, nq, width = wavefunction.shape
    size = x.shape[0] + 8
    return pl.pallas_call(
        functools.partial(exchange_body, num=num, vec_size=wavefunction.size), in_specs=[vmem, ANY], out_specs=[vmem, vmem],
        out_shape=[jax.ShapeDtypeStruct((num, size, 128), F32), jax.ShapeDtypeStruct((8, 128), F32)],
        scratch_shapes=[pltpu.VMEM((size, 128), F32), pltpu.VMEM((bond // num, nq, width), F32), pltpu.SemaphoreType.DMA((FIN_BLOCKS,))]
        + [pltpu.SemaphoreType.DMA((num - 1,))] * 2,
        compiler_params=pltpu.CompilerParams(collective_id=20, has_side_effects=True, vmem_limit_bytes=VMEM_LIMIT),
        name='exchange')(x, wavefunction)


def spread_body(me_ref, norm_ref, psi_ref, wide_ref, cur_ref, low_ref, turn_ref):
    nq, nb, _ = cur_ref.shape
    rows = pl.ds(pl.multiple_of(me_ref[0] * nb, 8), nb)
    norm = norm_ref[:1, :1]
    for q in range(nq):
        turn_ref[q % 2] = (psi_ref[:, q, :] / norm).T
        wide_ref[q] = turn_ref[q % 2].astype(BF16)
        own = turn_ref[q % 2, rows, :]
        cur_ref[q] = own
        low_ref[q] = own.astype(BF16)


def spread_call(wavefunction, norm_tile, me, slab):
    bond, nq, width = wavefunction.shape
    blk = 128
    return pl.pallas_call(
        spread_body,
        grid_spec=pltpu.PrefetchScalarGridSpec(
            num_scalar_prefetch=1, grid=(bond // blk,),
            in_specs=[pl.BlockSpec((8, 128), lambda i, m: (0, 0)), pl.BlockSpec((blk, nq, width), lambda i, m: (i, 0, 0))],
            out_specs=[pl.BlockSpec((nq, width, blk), lambda i, m: (0, 0, i)), pl.BlockSpec((nq, slab, blk), lambda i, m: (0, 0, i)),
                       pl.BlockSpec((nq, slab, blk), lambda i, m: (0, 0, i))],
            scratch_shapes=[pltpu.VMEM((2, width, blk), F32)]),
        out_shape=[jax.ShapeDtypeStruct((nq, width, bond), BF16), jax.ShapeDtypeStruct((nq, slab, bond), F32),
                   jax.ShapeDtypeStruct((nq, slab, bond), BF16)],
        compiler_params=pltpu.CompilerParams(dimension_semantics=('arbitrary',), vmem_limit_bytes=VMEM_LIMIT),
        cost_estimate=pl.CostEstimate(flops=wavefunction.size, bytes_accessed=8 * wavefunction.size, transcendentals=0),
        name='spread',
    )(me, norm_tile, wavefunction)


def sum_over_devices(slot_ref, value, send_sem, recv_sem, me, num):
    slot_ref[me] = value
    copies = []
    for off in range(1, num):
        peer = lax.rem(me + off, num)
        copies.append(pltpu.make_async_remote_copy(
            src_ref=slot_ref.at[me], dst_ref=slot_ref.at[me], send_sem=send_sem.at[off - 1], recv_sem=recv_sem.at[off - 1],
            device_id=(peer,), device_id_type=pl.DeviceIdType.MESH))
    for copy in copies:
        copy.start()
    for copy in copies:
        copy.wait()
    total = slot_ref[0]
    for src in range(1, num):
        total = total + slot_ref[src]
    return jnp.sum(total)


def fold(prod):
    rows, cols = prod.shape
    part = jnp.sum(prod.reshape(rows // 8, 8, cols), axis=0)
    out = part[:, :128]
    for i in range(1, cols // 128):
        out = out + part[:, i * 128:(i + 1) * 128]
    return out


def finish_body(beta_prev_ref, sigma_hbm, cur_hbm, prev_hbm, next_hbm, u0, u1, alpha_ref, beta_ref,
                sigma_ref, cur_ref, prev_ref, low_ref, slot_a, slot_b, in_sem, out_sem, send_a, recv_a, send_b, recv_b, *, num, vec_size):
    me = lax.axis_index(AXIS_NAME)
    nq, _, _ = sigma_ref.shape
    blk = nq // FIN_BLOCKS

    def load(n, i):
        src, dst = ((sigma_hbm, sigma_ref), (cur_hbm, cur_ref), (prev_hbm, prev_ref))[n]
        rows = pl.ds(i * blk, blk)
        return pltpu.make_async_copy(src.at[rows], dst.at[rows], in_sem.at[n, i])

    for i in range(FIN_BLOCKS):
        load(0, i).start()
        load(1, i).start()
    for i in range(FIN_BLOCKS):
        load(2, i).start()
    barrier = pltpu.get_barrier_semaphore()
    for off in range(1, num):
        pl.semaphore_signal(barrier, inc=1, device_id=(lax.rem(me + off, num),), device_id_type=pl.DeviceIdType.MESH)

    part = jnp.zeros((8, 128), F32)
    for i in range(FIN_BLOCKS):
        load(0, i).wait()
        load(1, i).wait()
        part = lax.fori_loop(i * blk, (i + 1) * blk, lambda q, acc: acc + fold(sigma_ref[q] * cur_ref[q]), part)
    pl.semaphore_wait(barrier, num - 1)
    alpha = sum_over_devices(slot_a, part, send_a, recv_a, me, num) / vec_size
    beta_prev = beta_prev_ref[0]
    for i in range(FIN_BLOCKS):
        load(2, i).wait()

    def residual_part(q, acc):
        res = sigma_ref[q] - alpha * cur_ref[q] - beta_prev * prev_ref[q]
        sigma_ref[q] = res
        return acc + fold(res * res)

    part = lax.fori_loop(0, nq, residual_part, jnp.zeros((8, 128), F32))
    norm = sum_over_devices(slot_b, part, send_b, recv_b, me, num) / vec_size
    beta_vec = jnp.sqrt(jnp.full((8, 128), norm, F32))
    alpha_ref[...] = jnp.full((8, 128), alpha, F32)
    beta_ref[...] = beta_vec
    beta_row = beta_vec[:1, :1]

    def scale_part(q, carry):
        nxt = sigma_ref[q] / beta_row
        cur_ref[q] = nxt
        low_ref[q] = nxt.astype(BF16)
        return carry

    def stores(i):
        rows = pl.ds(i * blk, blk)
        return [pltpu.make_async_copy(cur_ref.at[rows], next_hbm.at[rows], out_sem.at[0, i])] + [
            pltpu.make_async_copy(low_ref.at[rows, :, pl.ds(n * CHUNK, CHUNK)], ref.at[rows], out_sem.at[1 + n, i])
            for n, ref in enumerate((u0, u1))]

    for i in range(FIN_BLOCKS):
        lax.fori_loop(i * blk, (i + 1) * blk, scale_part, 0)
        for copy in stores(i):
            copy.start()
    for i in range(FIN_BLOCKS):
        for copy in stores(i):
            copy.wait()


def finish_call(beta_prev, sigma, cur, prev, num, vec_size, call_id):
    nq, nb, na = sigma.shape
    vmem = pl.BlockSpec(memory_space=pltpu.VMEM)
    return pl.pallas_call(
        functools.partial(finish_body, num=num, vec_size=vec_size),
        in_specs=[pl.BlockSpec(memory_space=pltpu.SMEM)] + [ANY] * 3,
        out_specs=[ANY] * 3 + [vmem] * 2,
        out_shape=[jax.ShapeDtypeStruct((nq, nb, na), F32)] + [jax.ShapeDtypeStruct((nq, nb, CHUNK), BF16)] * 2
        + [jax.ShapeDtypeStruct((8, 128), F32)] * 2,
        scratch_shapes=[pltpu.VMEM((nq, nb, na), F32)] * 3 + [pltpu.VMEM((nq, nb, na), BF16)] + [pltpu.VMEM((num, 8, 128), F32)] * 2
        + [pltpu.SemaphoreType.DMA((3, FIN_BLOCKS)), pltpu.SemaphoreType.DMA((3, FIN_BLOCKS))] + [pltpu.SemaphoreType.DMA((num - 1,))] * 4,
        compiler_params=pltpu.CompilerParams(collective_id=call_id, has_side_effects=True, vmem_limit_bytes=VMEM_LIMIT),
        cost_estimate=pl.CostEstimate(flops=10 * sigma.size, bytes_accessed=22 * sigma.size, transcendentals=0),
        name='finish',
    )(beta_prev, sigma, cur, prev)


def solution(mesh):
    num = mesh.shape[AXIS_NAME]

    def device_body(wavefunction, left_loc, pair_loc, right_loc, flag_loc):
        bond, nq, _ = wavefunction.shape
        vec_size = wavefunction.size
        slab = bond // num
        me = lax.axis_index(AXIS_NAME)
        nchunk = bond // CHUNK

        terms_loc = pair_loc.shape[0]
        small = jnp.concatenate([pair_loc.astype(F32).reshape(8, 128), jnp.pad(flag_loc.astype(F32), (0, 1024 - terms_loc)).reshape(8, 128)])
        small_all, norm_tile = exchange_call(small, wavefunction, num)
        right_slab = lax.all_to_all(right_loc, AXIS_NAME, split_axis=1, concat_axis=0, tiled=True)
        left_parts = []
        for i in range(nchunk):
            left_parts.append(lax.all_gather(left_loc[:, i * CHUNK:(i + 1) * CHUNK], AXIS_NAME, axis=0, tiled=True))
        pair_all = small_all[:, :8].reshape(num * terms_loc, nq, nq).astype(BF16)
        flags = small_all[:, 8, :terms_loc].reshape(-1).astype(jnp.int32)
        order = jnp.argsort(flags, stable=True).astype(jnp.int32)
        split = ((flags.shape[0] - jnp.sum(flags)) // GROUP).astype(jnp.int32).reshape(1)
        unit = (jnp.arange(slab)[:, None] + me * slab == jnp.arange(bond)[None, :]).astype(BF16)
        right_slab = jnp.where(flags[:, None, None] == 1, right_slab, unit[None])[order]
        eye = jnp.eye(ROW_TILE, dtype=BF16)
        pair_sorted = pair_all[order]
        pair_blk = (pair_sorted[:, :, None, :, None] * eye[None, None, :, None, :]).reshape(-1, nq * ROW_TILE, nq * ROW_TILE)

        here = me.reshape(1).astype(jnp.int32)
        krylov = first_call(wavefunction, norm_tile, here, slab, LANCZOS_STEPS + 1)
        u_wide, cur, cur_low = spread_call(wavefunction, norm_tile, here, slab)
        u_parts = [(cur_low, i) for i in range(nchunk)]
        u_wide = [(u_wide, i) for i in range(nchunk)]
        prev = jnp.zeros_like(cur)
        beta_prev = jnp.zeros((1,), F32)
        tiles = []
        leaving = arriving = None
        for step in range(LANCZOS_STEPS):
            if step == 0:
                sigma = None
                for i in range(nchunk):
                    sigma, krylov = one_sided_call(order, split, u_parts[i:i + 1], pair_blk, left_parts[i:i + 1], krylov, sigma)
                    sigma, krylov = full_call(order, split, *u_wide[i], right_slab, pair_blk, left_parts[i], sigma, krylov)
            else:
                if arriving is None:
                    sigma, krylov = one_sided_call(order, split, u_parts, pair_blk, left_parts, krylov)
                else:
                    sigma, arriving = one_sided_call(order, split, u_parts, pair_blk, left_parts, arriving)
                    krylov = place_call(arriving, krylov, step - 1)
                sigma, leaving = full_call(order, split, *u_wide[0], right_slab, pair_blk, left_parts[0], sigma, leaving)
                arriving = lax.all_to_all(leaving, AXIS_NAME, split_axis=0, concat_axis=0, tiled=False)
                sigma, krylov = full_call(order, split, *u_wide[1], right_slab, pair_blk, left_parts[1], sigma, krylov)
            nxt, *lows, alpha_t, beta_t = finish_call(beta_prev, sigma, cur, prev, num, vec_size, step)
            beta_prev = beta_t[0, :1]
            tiles += [alpha_t[0, :1], beta_prev]
            if step + 1 < LANCZOS_STEPS:
                u_parts = [(low, 0) for low in lows]
                u_wide = [(lax.all_gather(low, AXIS_NAME, axis=0, tiled=False), 0) for low in lows]
            prev, cur = cur, nxt
            leaving = nxt.reshape(nq * slab, bond).T.reshape(num, slab, nq * slab)
        krylov = place_call(arriving, krylov, LANCZOS_STEPS - 1)
        arriving = lax.all_to_all(leaving, AXIS_NAME, split_axis=0, concat_axis=0, tiled=False)
        krylov = place_call(arriving, krylov, LANCZOS_STEPS)
        scalars = jnp.concatenate(tiles)
        return krylov, scalars[0::2], scalars[1::2]

    return jax.shard_map(device_body, mesh=mesh, in_specs=(P(), P(AXIS_NAME), P(AXIS_NAME), P(AXIS_NAME), P(AXIS_NAME)), out_specs=(P(None, AXIS_NAME), P(), P()), check_vma=False)
```

```python
import functools

import jax
import jax.numpy as jnp
from jax import lax
from jax.experimental import pallas as pl
from jax.experimental.pallas import tpu as pltpu
from jax.sharding import PartitionSpec as P


LANCZOS_STEPS = 6
AXIS_NAME = 'terms'
GROUP = 4
CHUNK = 384
ROW_TILE = 16
BF16 = jnp.bfloat16
F32 = jnp.float32
FIN_BLOCKS = 4


def stacked_left(refs, cuts):
    rows, at = [], 0
    for cut in cuts:
        for t in range(GROUP):
            pieces = [refs[at + t * cut + k][0] for k in range(cut)]
            rows.append(pieces[0] if cut == 1 else jnp.concatenate(pieces, axis=1))
        at += GROUP * cut
    return jnp.concatenate(rows, axis=0)


def one_sided_body(order_ref, split_ref, *rest, cuts, resume):
    parts = len(cuts)
    u_refs = rest[:parts]
    pair_ref = rest[parts]
    left_refs = rest[parts + 1:parts + 1 + GROUP * sum(cuts)]
    rest = rest[parts + 1 + GROUP * sum(cuts):]
    if resume:
        sigma_in, rest = rest[0], rest[1:]
    rest = rest[1:]
    sigma_out, _, sigma_ref, z_ref, in_sem, out_sem = rest
    grp = pl.program_id(0)
    nq, nb, nc = u_refs[0].shape
    na = sigma_ref.shape[2]
    half = nq // 2
    last = jnp.maximum(split_ref[0] - 1, 0)

    @pl.when(grp == 0)
    def _():
        if resume:
            copy = pltpu.make_async_copy(sigma_in, sigma_ref, in_sem)
            copy.start()
            copy.wait()
        else:
            sigma_ref[...] = jnp.zeros_like(sigma_ref)

    @pl.when(grp < split_ref[0])
    def _():
        pair = pair_ref[...].reshape(GROUP * nq * ROW_TILE, nq * ROW_TILE)
        for ci in range(parts):
            for bt in range(0, nb // ROW_TILE, 2):
                rows = [pl.ds((bt + k) * ROW_TILE, ROW_TILE) for k in range(2)]
                y = jnp.concatenate([u_refs[ci][:, rows[k], :].reshape(nq * ROW_TILE, nc) for k in range(2)], axis=1)
                z = jnp.dot(pair, y, preferred_element_type=F32).astype(BF16)
                for k in range(2):
                    part = z[:, k * nc:(k + 1) * nc].reshape(GROUP, nq, ROW_TILE, nc)
                    for t in range(GROUP):
                        z_ref[:, rows[k], (ci * GROUP + t) * nc:(ci * GROUP + t + 1) * nc] = part[t]

    for h in range(2):
        @pl.when(grp < split_ref[0])
        def _():
            left = stacked_left(left_refs, cuts)
            zs = z_ref[h * half:(h + 1) * half].reshape(half * nb, parts * GROUP * nc)
            prod = jnp.dot(zs, left, preferred_element_type=F32).reshape(half, nb, na)
            sigma_ref[h * half:(h + 1) * half] += prod

        @pl.when(grp == last)
        def _():
            pltpu.make_async_copy(sigma_ref.at[pl.ds(h * half, half)], sigma_out.at[pl.ds(h * half, half)], out_sem.at[h]).start()

    @pl.when(grp == last)
    def _():
        for h in range(2):
            pltpu.make_async_copy(sigma_ref.at[pl.ds(h * half, half)], sigma_out.at[pl.ds(h * half, half)], out_sem.at[h]).wait()


def full_body(order_ref, split_ref, u_hbm, right_ref, pair_ref, *rest, gathered, chunk, cut):
    left_refs = rest[:GROUP * cut]
    sigma_in, _, sigma_out, _, sigma_ref, u_ref, y_ref, z_ref, u_sem, in_sem, out_sem = rest[GROUP * cut:]
    grp = pl.program_id(0)
    num_grp = pl.num_programs(0)
    nq, nb, na = sigma_ref.shape
    nd = right_ref.shape[2]
    nc = u_ref.shape[-1]
    half = nq // 2

    def u_copy(r):
        cols = pl.ds(chunk * nc, nc)
        if gathered:
            return pltpu.make_async_copy(u_hbm.at[:, r, :, cols], u_ref.at[:, r], u_sem.at[r])
        return pltpu.make_async_copy(u_hbm.at[r, :, cols], u_ref.at[r], u_sem.at[r])

    @pl.when((grp == 0) & (split_ref[0] < num_grp))
    def _():
        for r in range(nq):
            u_copy(r).start()
        pltpu.make_async_copy(sigma_in, sigma_ref, in_sem).start()

    def stage_right(first, last):
        right = right_ref[...].reshape(GROUP * nb, nd)
        for r in range(first, last, 2):
            u = jnp.concatenate([(u_ref[:, r + k] if gathered else u_ref[r + k]).reshape(nd, nc) for k in range(2)], axis=1)
            y = jnp.dot(right, u, preferred_element_type=F32).astype(BF16)
            for k in range(2):
                y_ref[r + k] = y[:, k * nc:(k + 1) * nc]

    head = nq // 4

    @pl.when(grp == split_ref[0])
    def _():
        for r in range(head):
            u_copy(r).wait()

    @pl.when(grp >= split_ref[0])
    def _():
        stage_right(0, head)

    @pl.when(grp == split_ref[0])
    def _():
        for r in range(head, nq):
            u_copy(r).wait()

    @pl.when(grp >= split_ref[0])
    def _():
        stage_right(head, nq)
        for t in range(GROUP):
            for bt in range(0, nb // ROW_TILE, 2):
                y = jnp.concatenate([y_ref[:, pl.ds(t * nb + (bt + k) * ROW_TILE, ROW_TILE), :].reshape(nq * ROW_TILE, nc) for k in range(2)], axis=1)
                z = jnp.dot(pair_ref[t], y, preferred_element_type=F32).astype(BF16)
                for k in range(2):
                    z_ref[:, pl.ds((bt + k) * ROW_TILE, ROW_TILE), t * nc:(t + 1) * nc] = z[:, k * nc:(k + 1) * nc].reshape(nq, ROW_TILE, nc)

    @pl.when(grp == split_ref[0])
    def _():
        pltpu.make_async_copy(sigma_in, sigma_ref, in_sem).wait()

    for h in range(2):
        @pl.when(grp >= split_ref[0])
        def _():
            left = stacked_left(left_refs, (cut,))
            zs = z_ref[h * half:(h + 1) * half].reshape(half * nb, GROUP * nc)
            prod = jnp.dot(zs, left, preferred_element_type=F32).reshape(half, nb, na)
            sigma_ref[h * half:(h + 1) * half] += prod

        @pl.when((grp == num_grp - 1) & (split_ref[0] < num_grp))
        def _():
            pltpu.make_async_copy(sigma_ref.at[pl.ds(h * half, half)], sigma_out.at[pl.ds(h * half, half)], out_sem.at[h]).start()

    @pl.when((grp == num_grp - 1) & (split_ref[0] < num_grp))
    def _():
        for h in range(2):
            pltpu.make_async_copy(sigma_ref.at[pl.ds(h * half, half)], sigma_out.at[pl.ds(h * half, half)], out_sem.at[h]).wait()


ANY = pl.BlockSpec(memory_space=pl.ANY)
VMEM_LIMIT = 63 << 20


def one_sided_call(order, split, u_parts, pair_blk, left_parts, carried, sigma=None):
    parts = len(u_parts)
    nq, nb, _ = u_parts[0][0].shape
    nc = CHUNK
    na = sum(piece.shape[2] for piece in left_parts[0])
    cuts = tuple(len(part) for part in left_parts)
    terms = pair_blk.shape[0]
    nk = nq * ROW_TILE

    def clamp(g, s):
        return jnp.minimum(g, jnp.maximum(s[0] - 1, 0))

    left_specs = [pl.BlockSpec((1,) + piece.shape[1:], functools.partial(lambda g, o, s, t: (o[clamp(g, s) * GROUP + t], 0, 0), t=t))
                  for part in left_parts for t in range(GROUP) for piece in part]
    resume = sigma is not None
    n = terms // 2
    first = 2 + parts + 1 + GROUP * sum(cuts)
    aliases = {first: 0, first + 1: 1} if resume else {first: 1}
    return pl.pallas_call(
        functools.partial(one_sided_body, cuts=cuts, resume=resume),
        grid_spec=pltpu.PrefetchScalarGridSpec(
            num_scalar_prefetch=2, grid=(terms // GROUP,),
            in_specs=[pl.BlockSpec((nq, nb, nc), functools.partial(lambda g, o, s, c: (0, 0, c), c=c), pipeline_mode=pl.Buffered(1)) for _, c in u_parts]
            + [pl.BlockSpec((GROUP, nk, nk), lambda g, o, s: (clamp(g, s), 0, 0))] + left_specs
            + [ANY] * (2 if resume else 1),
            out_specs=[ANY, ANY],
            scratch_shapes=[pltpu.VMEM((nq, nb, na), F32), pltpu.VMEM((nq, nb, parts * GROUP * nc), BF16),
                            pltpu.SemaphoreType.DMA, pltpu.SemaphoreType.DMA((2,))]),
        out_shape=[jax.ShapeDtypeStruct((nq, nb, na), F32), jax.ShapeDtypeStruct(carried.shape, carried.dtype)],
        input_output_aliases=aliases,
        compiler_params=pltpu.CompilerParams(dimension_semantics=('arbitrary',), vmem_limit_bytes=VMEM_LIMIT),
        cost_estimate=pl.CostEstimate(flops=n * 2 * nq * nb * parts * nc * (na + nk), bytes_accessed=n * na * nc * parts * 2, transcendentals=0),
        name='one_sided',
    )(order, split, *[u for u, _ in u_parts], pair_blk, *[piece for part in left_parts for _ in range(GROUP) for piece in part], *([sigma] if resume else []), carried)


def full_call(order, split, u_part, chunk, right_slab, pair_blk, left_part, sigma, carried):
    nq, nb, na = sigma.shape
    nc = CHUNK
    terms, _, nd = right_slab.shape
    nk = nq * ROW_TILE

    def at_least(g, s):
        return jnp.minimum(jnp.maximum(g, s[0]), terms // GROUP - 1)

    left_specs = [pl.BlockSpec((1,) + piece.shape[1:], functools.partial(lambda g, o, s, t: (o[at_least(g, s) * GROUP + t], 0, 0), t=t))
                  for t in range(GROUP) for piece in left_part]
    cut = len(left_part)
    n = terms // 2
    return pl.pallas_call(
        functools.partial(full_body, gathered=u_part.ndim == 4, chunk=chunk, cut=cut),
        grid_spec=pltpu.PrefetchScalarGridSpec(
            num_scalar_prefetch=2, grid=(terms // GROUP,),
            in_specs=[ANY,
                      pl.BlockSpec((GROUP, nb, nd), lambda g, o, s: (at_least(g, s), 0, 0)),
                      pl.BlockSpec((GROUP, nk, nk), lambda g, o, s: (at_least(g, s), 0, 0))] + left_specs + [ANY, ANY],
            out_specs=[ANY, ANY],
            scratch_shapes=[pltpu.VMEM((nq, nb, na), F32), pltpu.VMEM(u_part.shape[:-1] + (nc,), BF16),
                            pltpu.VMEM((nq, GROUP * nb, nc), BF16), pltpu.VMEM((nq, nb, GROUP * nc), BF16),
                            pltpu.SemaphoreType.DMA((nq,)), pltpu.SemaphoreType.DMA, pltpu.SemaphoreType.DMA((2,))]),
        out_shape=[jax.ShapeDtypeStruct((nq, nb, na), F32), jax.ShapeDtypeStruct(carried.shape, carried.dtype)],
        input_output_aliases={2 + 3 + GROUP * cut: 0, 2 + 4 + GROUP * cut: 1},
        compiler_params=pltpu.CompilerParams(dimension_semantics=('arbitrary',), vmem_limit_bytes=VMEM_LIMIT),
        cost_estimate=pl.CostEstimate(flops=n * 2 * nq * nb * nc * (nd + na + nk), bytes_accessed=n * na * nc * 2 + nq * nd * nc * 2, transcendentals=0),
        name='full_terms',
    )(order, split, u_part, right_slab, pair_blk, *left_part * GROUP, sigma, carried)


def place_body(*refs, num, nq, width):
    x_ref, out_ref = refs[0], refs[-1]
    for q0 in range(0, nq, 8):
        lines = [jnp.concatenate([x_ref[src, :, q * width:(q + 1) * width] for src in range(num)], axis=1) for q in range(q0, q0 + 8)]
        out_ref[0, :, q0:q0 + 8, :] = jnp.swapaxes(jnp.stack(lines, axis=0), 0, 1)


def place_call(arrived, krylov, index):
    num, rows, size = arrived.shape
    nq, wide = krylov.shape[2:]
    blk = rows // 4
    return pl.pallas_call(
        functools.partial(place_body, num=num, nq=nq, width=wide // num),
        grid=(4,),
        in_specs=[pl.BlockSpec((num, blk, size), lambda i: (0, i, 0)), ANY],
        out_specs=pl.BlockSpec((1, blk, nq, wide), lambda i: (index, i, 0, 0)),
        out_shape=jax.ShapeDtypeStruct(krylov.shape, krylov.dtype),
        input_output_aliases={1: 0},
        compiler_params=pltpu.CompilerParams(dimension_semantics=('arbitrary',), vmem_limit_bytes=VMEM_LIMIT),
        cost_estimate=pl.CostEstimate(flops=0, bytes_accessed=8 * arrived.size, transcendentals=0),
        name='place',
    )(arrived, krylov)


def first_body(me_ref, norm_ref, psi_ref, out_ref):
    out_ref[0] = psi_ref[...] / norm_ref[:1, :1]


def first_call(wavefunction, norm_tile, me, rows, count):
    _, nq, width = wavefunction.shape
    blk = rows // 4
    return pl.pallas_call(
        first_body,
        grid_spec=pltpu.PrefetchScalarGridSpec(
            num_scalar_prefetch=1, grid=(4,),
            in_specs=[pl.BlockSpec((8, 128), lambda i, m: (0, 0)), pl.BlockSpec((blk, nq, width), lambda i, m: (m[0] * 4 + i, 0, 0))],
            out_specs=pl.BlockSpec((1, blk, nq, width), lambda i, m: (0, i, 0, 0))),
        out_shape=jax.ShapeDtypeStruct((count, rows, nq, width), F32),
        compiler_params=pltpu.CompilerParams(dimension_semantics=('arbitrary',), vmem_limit_bytes=VMEM_LIMIT),
        cost_estimate=pl.CostEstimate(flops=rows * nq * width, bytes_accessed=8 * rows * nq * width, transcendentals=0),
        name='first',
    )(me, norm_tile, wavefunction)


def exchange_body(x_ref, psi_hbm, out_ref, norm_ref, stage_ref, psi_ref, psi_sem, send_sem, recv_sem, *, num, vec_size):
    me = lax.axis_index(AXIS_NAME)
    rows = psi_ref.shape[0]
    blk = rows // FIN_BLOCKS
    small = x_ref.shape[0]

    def load(i):
        return pltpu.make_async_copy(psi_hbm.at[pl.ds(me * rows + i * blk, blk)], psi_ref.at[pl.ds(i * blk, blk)], psi_sem.at[i])

    for i in range(FIN_BLOCKS):
        load(i).start()
    barrier = pltpu.get_barrier_semaphore()
    for off in range(1, num):
        pl.semaphore_signal(barrier, inc=1, device_id=(lax.rem(me + off, num),), device_id_type=pl.DeviceIdType.MESH)
    stage_ref[:small] = x_ref[...]
    part = jnp.zeros((8, 128), F32)
    for i in range(FIN_BLOCKS):
        load(i).wait()
        part = lax.fori_loop(i * blk, (i + 1) * blk, lambda a, acc: acc + fold(psi_ref[a] * psi_ref[a]), part)
    stage_ref[small:] = part
    pl.semaphore_wait(barrier, num - 1)
    copies = []
    for off in range(1, num):
        copies.append(pltpu.make_async_remote_copy(
            src_ref=stage_ref, dst_ref=out_ref.at[me], send_sem=send_sem.at[off - 1], recv_sem=recv_sem.at[off - 1],
            device_id=(lax.rem(me + off, num),), device_id_type=pl.DeviceIdType.MESH))
    for copy in copies:
        copy.start()
    out_ref[me] = stage_ref[...]
    for copy in copies:
        copy.wait()
    total = out_ref[0, small:]
    for src in range(1, num):
        total = total + out_ref[src, small:]
    norm_ref[...] = jnp.sqrt(jnp.full((8, 128), jnp.sum(total) / vec_size, F32))


def exchange_call(x, wavefunction, num):
    vmem = pl.BlockSpec(memory_space=pltpu.VMEM)
    bond, nq, width = wavefunction.shape
    size = x.shape[0] + 8
    return pl.pallas_call(
        functools.partial(exchange_body, num=num, vec_size=wavefunction.size), in_specs=[vmem, ANY], out_specs=[vmem, vmem],
        out_shape=[jax.ShapeDtypeStruct((num, size, 128), F32), jax.ShapeDtypeStruct((8, 128), F32)],
        scratch_shapes=[pltpu.VMEM((size, 128), F32), pltpu.VMEM((bond // num, nq, width), F32), pltpu.SemaphoreType.DMA((FIN_BLOCKS,))]
        + [pltpu.SemaphoreType.DMA((num - 1,))] * 2,
        compiler_params=pltpu.CompilerParams(collective_id=20, has_side_effects=True, vmem_limit_bytes=VMEM_LIMIT),
        name='exchange')(x, wavefunction)


def spread_body(me_ref, norm_ref, psi_ref, wide_ref, cur_ref, low_ref, turn_ref):
    nq, nb, _ = cur_ref.shape
    rows = pl.ds(pl.multiple_of(me_ref[0] * nb, 8), nb)
    norm = norm_ref[:1, :1]
    for q in range(nq):
        turn_ref[q % 2] = (psi_ref[:, q, :] / norm).T
        wide_ref[q] = turn_ref[q % 2].astype(BF16)
        own = turn_ref[q % 2, rows, :]
        cur_ref[q] = own
        low_ref[q] = own.astype(BF16)


def spread_call(wavefunction, norm_tile, me, slab):
    bond, nq, width = wavefunction.shape
    blk = 128
    return pl.pallas_call(
        spread_body,
        grid_spec=pltpu.PrefetchScalarGridSpec(
            num_scalar_prefetch=1, grid=(bond // blk,),
            in_specs=[pl.BlockSpec((8, 128), lambda i, m: (0, 0)), pl.BlockSpec((blk, nq, width), lambda i, m: (i, 0, 0))],
            out_specs=[pl.BlockSpec((nq, width, blk), lambda i, m: (0, 0, i)), pl.BlockSpec((nq, slab, blk), lambda i, m: (0, 0, i)),
                       pl.BlockSpec((nq, slab, blk), lambda i, m: (0, 0, i))],
            scratch_shapes=[pltpu.VMEM((2, width, blk), F32)]),
        out_shape=[jax.ShapeDtypeStruct((nq, width, bond), BF16), jax.ShapeDtypeStruct((nq, slab, bond), F32),
                   jax.ShapeDtypeStruct((nq, slab, bond), BF16)],
        compiler_params=pltpu.CompilerParams(dimension_semantics=('arbitrary',), vmem_limit_bytes=VMEM_LIMIT),
        cost_estimate=pl.CostEstimate(flops=wavefunction.size, bytes_accessed=8 * wavefunction.size, transcendentals=0),
        name='spread',
    )(me, norm_tile, wavefunction)


def sum_over_devices(slot_ref, value, send_sem, recv_sem, me, num):
    slot_ref[me] = value
    copies = []
    for off in range(1, num):
        peer = lax.rem(me + off, num)
        copies.append(pltpu.make_async_remote_copy(
            src_ref=slot_ref.at[me], dst_ref=slot_ref.at[me], send_sem=send_sem.at[off - 1], recv_sem=recv_sem.at[off - 1],
            device_id=(peer,), device_id_type=pl.DeviceIdType.MESH))
    for copy in copies:
        copy.start()
    for copy in copies:
        copy.wait()
    total = slot_ref[0]
    for src in range(1, num):
        total = total + slot_ref[src]
    return jnp.sum(total)


def fold(prod):
    rows, cols = prod.shape
    part = jnp.sum(prod.reshape(rows // 8, 8, cols), axis=0)
    out = part[:, :128]
    for i in range(1, cols // 128):
        out = out + part[:, i * 128:(i + 1) * 128]
    return out


def finish_body(beta_prev_ref, sigma_hbm, cur_hbm, prev_hbm, next_hbm, u0, u1, alpha_ref, beta_ref,
                sigma_ref, cur_ref, prev_ref, low_ref, slot_a, slot_b, in_sem, out_sem, send_a, recv_a, send_b, recv_b, *, num, vec_size):
    me = lax.axis_index(AXIS_NAME)
    nq, _, _ = sigma_ref.shape
    blk = nq // FIN_BLOCKS

    def load(n, i):
        src, dst = ((sigma_hbm, sigma_ref), (cur_hbm, cur_ref), (prev_hbm, prev_ref))[n]
        rows = pl.ds(i * blk, blk)
        return pltpu.make_async_copy(src.at[rows], dst.at[rows], in_sem.at[n, i])

    for i in range(FIN_BLOCKS):
        load(0, i).start()
        load(1, i).start()
    for i in range(FIN_BLOCKS):
        load(2, i).start()
    barrier = pltpu.get_barrier_semaphore()
    for off in range(1, num):
        pl.semaphore_signal(barrier, inc=1, device_id=(lax.rem(me + off, num),), device_id_type=pl.DeviceIdType.MESH)

    part = jnp.zeros((8, 128), F32)
    for i in range(FIN_BLOCKS):
        load(0, i).wait()
        load(1, i).wait()
        part = lax.fori_loop(i * blk, (i + 1) * blk, lambda q, acc: acc + fold(sigma_ref[q] * cur_ref[q]), part)
    pl.semaphore_wait(barrier, num - 1)
    alpha = sum_over_devices(slot_a, part, send_a, recv_a, me, num) / vec_size
    beta_prev = beta_prev_ref[0]
    for i in range(FIN_BLOCKS):
        load(2, i).wait()

    def residual_part(q, acc):
        res = sigma_ref[q] - alpha * cur_ref[q] - beta_prev * prev_ref[q]
        sigma_ref[q] = res
        return acc + fold(res * res)

    part = lax.fori_loop(0, nq, residual_part, jnp.zeros((8, 128), F32))
    norm = sum_over_devices(slot_b, part, send_b, recv_b, me, num) / vec_size
    beta_vec = jnp.sqrt(jnp.full((8, 128), norm, F32))
    alpha_ref[...] = jnp.full((8, 128), alpha, F32)
    beta_ref[...] = beta_vec
    beta_row = beta_vec[:1, :1]

    def scale_part(q, carry):
        nxt = sigma_ref[q] / beta_row
        cur_ref[q] = nxt
        low_ref[q] = nxt.astype(BF16)
        return carry

    def stores(i):
        rows = pl.ds(i * blk, blk)
        return [pltpu.make_async_copy(cur_ref.at[rows], next_hbm.at[rows], out_sem.at[0, i])] + [
            pltpu.make_async_copy(low_ref.at[rows, :, pl.ds(n * CHUNK, CHUNK)], ref.at[rows], out_sem.at[1 + n, i])
            for n, ref in enumerate((u0, u1))]

    for i in range(FIN_BLOCKS):
        lax.fori_loop(i * blk, (i + 1) * blk, scale_part, 0)
        for copy in stores(i):
            copy.start()
    for i in range(FIN_BLOCKS):
        for copy in stores(i):
            copy.wait()


def finish_call(beta_prev, sigma, cur, prev, num, vec_size, call_id):
    nq, nb, na = sigma.shape
    vmem = pl.BlockSpec(memory_space=pltpu.VMEM)
    return pl.pallas_call(
        functools.partial(finish_body, num=num, vec_size=vec_size),
        in_specs=[pl.BlockSpec(memory_space=pltpu.SMEM)] + [ANY] * 3,
        out_specs=[ANY] * 3 + [vmem] * 2,
        out_shape=[jax.ShapeDtypeStruct((nq, nb, na), F32)] + [jax.ShapeDtypeStruct((nq, nb, CHUNK), BF16)] * 2
        + [jax.ShapeDtypeStruct((8, 128), F32)] * 2,
        scratch_shapes=[pltpu.VMEM((nq, nb, na), F32)] * 3 + [pltpu.VMEM((nq, nb, na), BF16)] + [pltpu.VMEM((num, 8, 128), F32)] * 2
        + [pltpu.SemaphoreType.DMA((3, FIN_BLOCKS)), pltpu.SemaphoreType.DMA((3, FIN_BLOCKS))] + [pltpu.SemaphoreType.DMA((num - 1,))] * 4,
        compiler_params=pltpu.CompilerParams(collective_id=call_id, has_side_effects=True, vmem_limit_bytes=VMEM_LIMIT),
        cost_estimate=pl.CostEstimate(flops=10 * sigma.size, bytes_accessed=22 * sigma.size, transcendentals=0),
        name='finish',
    )(beta_prev, sigma, cur, prev)


def solution(mesh):
    num = mesh.shape[AXIS_NAME]

    def device_body(wavefunction, left_loc, pair_loc, right_loc, flag_loc):
        bond, nq, _ = wavefunction.shape
        vec_size = wavefunction.size
        slab = bond // num
        me = lax.axis_index(AXIS_NAME)
        nchunk = 2

        terms_loc = pair_loc.shape[0]
        small = jnp.concatenate([pair_loc.astype(F32).reshape(8, 128), jnp.pad(flag_loc.astype(F32), (0, 1024 - terms_loc)).reshape(8, 128)])
        small_all, norm_tile = exchange_call(small, wavefunction, num)
        right_slab = lax.all_to_all(right_loc, AXIS_NAME, split_axis=1, concat_axis=0, tiled=True)
        top = lax.all_gather(left_loc[:, :CHUNK], AXIS_NAME, axis=0, tiled=True)
        corner = lax.all_gather(left_loc[:, CHUNK:, CHUNK:], AXIS_NAME, axis=0, tiled=True)
        left_parts = [(top,), (top[:, :, CHUNK:].transpose(0, 2, 1), corner)]
        pair_all = small_all[:, :8].reshape(num * terms_loc, nq, nq).astype(BF16)
        flags = small_all[:, 8, :terms_loc].reshape(-1).astype(jnp.int32)
        order = jnp.argsort(flags, stable=True).astype(jnp.int32)
        split = ((flags.shape[0] - jnp.sum(flags)) // GROUP).astype(jnp.int32).reshape(1)
        unit = (jnp.arange(slab)[:, None] + me * slab == jnp.arange(bond)[None, :]).astype(BF16)
        right_slab = jnp.where(flags[:, None, None] == 1, right_slab, unit[None])[order]
        eye = jnp.eye(ROW_TILE, dtype=BF16)
        pair_sorted = pair_all[order]
        pair_blk = (pair_sorted[:, :, None, :, None] * eye[None, None, :, None, :]).reshape(-1, nq * ROW_TILE, nq * ROW_TILE)

        here = me.reshape(1).astype(jnp.int32)
        krylov = first_call(wavefunction, norm_tile, here, slab, LANCZOS_STEPS + 1)
        u_wide, cur, cur_low = spread_call(wavefunction, norm_tile, here, slab)
        u_parts = [(cur_low, i) for i in range(nchunk)]
        u_wide = [(u_wide, i) for i in range(nchunk)]
        prev = jnp.zeros_like(cur)
        beta_prev = jnp.zeros((1,), F32)
        tiles = []
        leaving = arriving = None
        sigma, krylov = one_sided_call(order, split, u_parts[:1], pair_blk, left_parts[:1], krylov)
        for step in range(LANCZOS_STEPS):
            if step == 0:
                for i in range(nchunk):
                    if i:
                        sigma, krylov = one_sided_call(order, split, u_parts[i:i + 1], pair_blk, left_parts[i:i + 1], krylov, sigma)
                    sigma, krylov = full_call(order, split, *u_wide[i], right_slab, pair_blk, left_parts[i], sigma, krylov)
            else:
                if arriving is None:
                    sigma, krylov = one_sided_call(order, split, u_parts, pair_blk, left_parts, krylov)
                else:
                    sigma, arriving = one_sided_call(order, split, u_parts, pair_blk, left_parts, arriving)
                    krylov = place_call(arriving, krylov, step - 1)
                sigma, leaving = full_call(order, split, *u_wide[0], right_slab, pair_blk, left_parts[0], sigma, leaving)
                arriving = lax.all_to_all(leaving, AXIS_NAME, split_axis=0, concat_axis=0, tiled=False)
                sigma, krylov = full_call(order, split, *u_wide[1], right_slab, pair_blk, left_parts[1], sigma, krylov)
            nxt, *lows, alpha_t, beta_t = finish_call(beta_prev, sigma, cur, prev, num, vec_size, step)
            beta_prev = beta_t[0, :1]
            tiles += [alpha_t[0, :1], beta_prev]
            if step + 1 < LANCZOS_STEPS:
                u_parts = [(low, 0) for low in lows]
                u_wide = [(lax.all_gather(low, AXIS_NAME, axis=0, tiled=False), 0) for low in lows]
            prev, cur = cur, nxt
            leaving = nxt.reshape(nq * slab, bond).T.reshape(num, slab, nq * slab)
        krylov = place_call(arriving, krylov, LANCZOS_STEPS - 1)
        arriving = lax.all_to_all(leaving, AXIS_NAME, split_axis=0, concat_axis=0, tiled=False)
        krylov = place_call(arriving, krylov, LANCZOS_STEPS)
        scalars = jnp.concatenate(tiles)
        return krylov, scalars[0::2], scalars[1::2]

    return jax.shard_map(device_body, mesh=mesh, in_specs=(P(), P(AXIS_NAME), P(AXIS_NAME), P(AXIS_NAME), P(AXIS_NAME)), out_specs=(P(None, AXIS_NAME), P(), P()), check_vma=False)
```
